32 devices in a mesh: row: 8 (over z, x), col: 4 (over y, core).
Axes of the slice: x: 2, y: 2, z: 4, core: 2. Of those that a mesh axis runs over, the one named last changes fastest.
Arguments:
- old_params: float32 [2, 64, 131072], P(None, ('row', 'col')), may hold values from -0.12 to 0.12
- old_first: float32 [2, 64, 131072], P(None, ('row', 'col')), may hold values from -1.8 to 1.8
- old_second: float32 [2, 64, 131072], P(None, ('row', 'col')), may hold values from 0.001 to 1
- gradients: float32 [2, 32, 262144], P(None, ('row', 'col')), may hold values from -250 to 250
- old_table: int32 [2, 64], replicated, may hold values from 0 to 63, as said below
- new_table: int32 [2, 32], replicated, may hold values from 0 to 31, as said below
Outputs:
- new_params: float32 [2, 32, 262144], P(None, ('row', 'col'))
- new_first: float32 [2, 32, 262144], P(None, ('row', 'col'))
- new_second: float32 [2, 32, 262144], P(None, ('row', 'col'))
The draws below stay inside these ranges and needn't reach their ends.
Inputs may be any that keep to these rules, and one draw needn't show every extreme that they name: old_table[t, p] = p XOR k for one k per tensor. new_table[t, q] = q XOR k for one k per tensor.
All inputs are finite; a program needn't handle non-finite values.
Results may differ from the reference program's by a relative error of at most 0.00002.
Values sent between devices are 32-bit elements; how exact they have to be, the bound alone decides.
No kernel may reach another device: no remote copies, remote signals or barrier semaphores. Data moves between devices by JAX's collectives and lax.ppermute only.
A program may use at most 64 MiB of HBM per device.

```python
import math
import jax
import jax.numpy as jnp

STEP = 100
NT = 2
ELEMS = 8388608
OLD_SHARDS = 64
OB = 131072
DEVICES = 32


def draw_old_table(key, part):
    folded = jax.random.fold_in(key, 11)
    offsets = jax.random.randint(folded, (NT, 1), 0, OLD_SHARDS)
    return jnp.bitwise_xor(jnp.arange(OLD_SHARDS, dtype=jnp.int32)[None, :], offsets).astype(jnp.int32)


def draw_new_table(key, part):
    folded = jax.random.fold_in(key, 23)
    offsets = jax.random.randint(folded, (NT, 1), 0, DEVICES)
    return jnp.bitwise_xor(jnp.arange(DEVICES, dtype=jnp.int32)[None, :], offsets).astype(jnp.int32)


def draw_gradients(key, part):
    folded = jax.random.fold_in(key, 37)
    key_private = jax.random.fold_in(folded, 0)
    position = jnp.arange(DEVICES, dtype=jnp.float32)[None, :, None]
    rising = 1.0 + 2.0 * position / max(DEVICES - 1, 1)
    private = jnp.clip(jax.random.normal(key_private, (NT, DEVICES, 2 * OB)), -8.0, 8.0)
    return (rising * private).astype(jnp.float32)


def shard_levels(own_key, shape, cuts, smallest, top_value):
    factor_of, own = 1.0, jax.random.fold_in(own_key, 6)
    for axis_at, parts in cuts:
        draws = jnp.exp(jax.random.uniform(jax.random.fold_in(own, axis_at), (parts,), jnp.float32, smallest / len(cuts), top_value / len(cuts)))
        factor_of = factor_of * jnp.repeat(draws, shape[axis_at] // parts).reshape([-1 if axis == axis_at else 1 for axis in range(len(shape))])
    return factor_of


def noise(key, shape, spread, most, cuts=(), held_as=jnp.bfloat16):
    gain = shard_levels(key, shape, cuts, -0.22, 0.18) if cuts else 1.0
    entries = jax.random.normal(key, shape, jnp.float32) * spread * gain
    return jnp.minimum(jnp.maximum(entries, -most), most).astype(held_as)


def setup_inputs(seed: int = 0) -> dict:
    seeds = jax.random.split(jax.random.key(seed), 7)
    return {
        "old_params": noise(seeds[0], (NT, OLD_SHARDS, OB), 0.02, 0.12, ((1, 32),), jnp.float32),
        "old_first": noise(seeds[1], (NT, OLD_SHARDS, OB), 0.3, 1.8, ((1, 32),), jnp.float32),
        "old_second": jnp.clip(jnp.exp(math.log(1.0) - 6.9077552 * jax.random.uniform(seeds[2], (NT, OLD_SHARDS, OB), jnp.float32) ** shard_levels(seeds[2], (NT, OLD_SHARDS, OB), ((1, 32),), -0.2, 0.2)), 0.001, 1.0),
        "gradients": draw_gradients(jax.random.fold_in(seeds[6], 71), 0),
        "old_table": draw_old_table(jax.random.fold_in(seeds[6], 71), 0),
        "new_table": draw_new_table(jax.random.fold_in(seeds[6], 71), 0),
    }


beta_one = 0.9
beta_two = 0.95
epsilon = 1e-08
learn_rate = 0.001
decay_rate = 0.1

def relayout(old_state, old_table, new_table):
    tensors = jnp.arange(old_state.shape[0], dtype=jnp.int32)[:, None]
    blocks = jnp.zeros_like(old_state).at[tensors, old_table].set(old_state)
    paired = blocks.reshape(old_state.shape[0], old_state.shape[1] // 2, 2 * old_state.shape[2])
    return paired[tensors, new_table]

def adam_update(params, first_moment, second_moment, gradients, clip_factor):
    scaled = clip_factor * gradients
    first_new = beta_one * first_moment + (1.0 - beta_one) * scaled
    second_new = beta_two * second_moment + (1.0 - beta_two) * scaled * scaled
    bias_first = 1.0 - beta_one ** STEP
    bias_second = 1.0 - beta_two ** STEP
    update = first_new / bias_first / (jnp.sqrt(second_new / bias_second) + epsilon)
    params_new = params - learn_rate * (update + decay_rate * params)
    return (params_new, first_new, second_new)

def reference(old_params, old_first, old_second, gradients, old_table, new_table):
    moved_params = relayout(old_params, old_table, new_table)
    moved_first = relayout(old_first, old_table, new_table)
    moved_second = relayout(old_second, old_table, new_table)
    grad_norm = jnp.sqrt(jnp.sum(gradients * gradients))
    limit = jnp.float32(0.5 * (NT * ELEMS) ** 0.5)
    clip_factor = limit / jnp.maximum(grad_norm, limit)
    return adam_update(moved_params, moved_first, moved_second, gradients, clip_factor)
```

```python
import math

import jax
import jax.numpy as jnp
from jax import lax
from jax.experimental import pallas as pl
from jax.experimental.pallas import tpu as pltpu
from jax.sharding import PartitionSpec as P

STEP = 100
LANES = 128
ROWS = 512
GROUP_BITS = 5

beta_one = 0.9
beta_two = 0.95
epsilon = 1e-08
learn_rate = 0.001
decay_rate = 0.1
AXES = ("row", "col")


def adam_body(low_ref, clip_ref, p_ref, m_ref, v_ref, g_ref, *refs):
    np_ref, nm_ref, nv_ref = refs[-3:]
    rows = g_ref.shape[2]
    low = low_ref[0] == 1
    clip = clip_ref[0]
    inv_first = 1.0 / (1.0 - beta_one**STEP)
    inv_second = 1.0 / (1.0 - beta_two**STEP)

    def halves(ref):
        even = ref[pl.ds(0, rows, stride=2), :]
        odd = ref[pl.ds(1, rows, stride=2), :]
        return jnp.where(low, odd, even), jnp.where(low, even, odd)

    ps, ms, vs = halves(p_ref), halves(m_ref), halves(v_ref)
    for half in range(2):
        scaled = clip * g_ref[0, half]
        first_new = beta_one * ms[half] + (1.0 - beta_one) * scaled
        second_new = beta_two * vs[half] + (1.0 - beta_two) * scaled * scaled
        update = first_new * inv_first / (jnp.sqrt(second_new * inv_second) + epsilon)
        np_ref[0, half] = ps[half] - learn_rate * (update + decay_rate * ps[half])
        nm_ref[0, half] = first_new
        nv_ref[0, half] = second_new


def adam_tensor(tensor, state, grads, low, clip, partial=None):
    count = grads.shape[2]
    rows = math.gcd(count, ROWS)
    smem = pl.BlockSpec(memory_space=pltpu.SMEM)
    moved = pl.BlockSpec((2 * rows, LANES), lambda j: (j, 0))
    fresh = pl.BlockSpec((1, 2, rows, LANES), lambda j: (tensor, 0, j, 0))
    kept = list(partial) if partial is not None else []
    return pl.pallas_call(
        adam_body,
        grid=(count // rows,),
        in_specs=[smem, smem, moved, moved, moved, fresh] + [pl.BlockSpec(memory_space=pl.ANY)] * len(kept),
        out_specs=[fresh] * 3,
        out_shape=[jax.ShapeDtypeStruct(grads.shape, grads.dtype)] * 3,
        input_output_aliases={6 + i: i for i in range(len(kept))},
        compiler_params=pltpu.CompilerParams(dimension_semantics=("arbitrary",)),
        name=f"adam_{tensor}",
    )(low.reshape(1), clip.reshape(1), *state, grads, *kept)


def moved_by(key, arrays):
    if key == 0:
        return tuple(arrays)
    pairs = [(i, i ^ key) for i in range(lax.axis_size(AXES))]
    return tuple(lax.ppermute(a, AXES, pairs) for a in arrays)


def clip_of(grads):
    total = lax.psum(jnp.sum(grads * grads), AXES)
    limit = jnp.float32(0.5 * math.sqrt(grads.size * lax.axis_size(AXES)))
    return limit / jnp.maximum(jnp.sqrt(total), limit)


def shards(old_params, old_first, old_second, gradients, old_table, new_table):
    devices = lax.axis_size(AXES)
    tensors, halves, length = old_params.shape
    count = length // LANES
    old_key = old_table[:, 0]
    route = jnp.bitwise_xor(jnp.right_shift(old_key, 1), new_table[:, 0])
    low = jnp.bitwise_and(old_key, 1)
    grads = gradients.reshape(tensors, halves, count, LANES)

    def rows_of(a):
        return a.reshape(tensors, halves, count, LANES).transpose(0, 2, 1, 3).reshape(tensors, count * halves, LANES)

    state = [rows_of(a) for a in (old_params, old_first, old_second)]

    def first_move(key):
        def branch(mine, values):
            return moved_by(key, mine), clip_of(values)
        return branch

    bits = devices.bit_length() - 1
    rest = [(at, min(GROUP_BITS, bits - at)) for at in range(GROUP_BITS, bits, GROUP_BITS)]
    first = min(GROUP_BITS, bits)

    def field(t, at, width):
        return jnp.bitwise_and(jnp.right_shift(route[t], at), (1 << width) - 1)

    def rest_of_way(t, mine):
        for at, width in rest:
            hops = [lambda arrays, key=key: moved_by(key << at, arrays) for key in range(1 << width)]
            mine = lax.switch(field(t, at, width), hops, mine)
        return mine

    got, clip = lax.switch(field(0, 0, first), [first_move(k) for k in range(1 << first)], [s[0] for s in state], grads)
    got = rest_of_way(0, got)
    partial = None
    for t in range(1, tensors):
        def next_move(key, t=t, partial=partial):
            def branch(mine, ready, values, clip):
                return moved_by(key, mine), adam_tensor(t - 1, ready, values, low[t - 1], clip, partial)
            return branch

        got, partial = lax.switch(field(t, 0, first), [next_move(k) for k in range(1 << first)], [s[t] for s in state], got, grads, clip)
        got = rest_of_way(t, got)
    outs = adam_tensor(tensors - 1, got, grads, low[tensors - 1], clip, partial)
    return tuple(o.reshape(gradients.shape) for o in outs)


def solution(mesh):
    spec = P(None, AXES, None)
    return jax.shard_map(
        shards,
        mesh=mesh,
        in_specs=(spec, spec, spec, spec, P(), P()),
        out_specs=(spec, spec, spec),
        check_vma=False,
    )
```

```python
import math

import jax
import jax.numpy as jnp
from jax import lax
from jax.experimental import pallas as pl
from jax.experimental.pallas import tpu as pltpu
from jax.sharding import PartitionSpec as P

STEP = 100
LANES = 128
ROWS = 512
GROUP_BITS = 5

beta_one = 0.9
beta_two = 0.95
epsilon = 1e-08
learn_rate = 0.001
decay_rate = 0.1
AXES = ("row", "col")


def adam_body(low_ref, clip_ref, p_ref, m_ref, v_ref, g_ref, *refs):
    np_ref, nm_ref, nv_ref = refs[-3:]
    rows = g_ref.shape[2]
    low = low_ref[0] == 1
    clip = clip_ref[0]
    inv_first = 1.0 / (1.0 - beta_one**STEP)
    inv_second = 1.0 / (1.0 - beta_two**STEP)

    def halves(ref):
        even = ref[pl.ds(0, rows, stride=2), :]
        odd = ref[pl.ds(1, rows, stride=2), :]
        return jnp.where(low, odd, even), jnp.where(low, even, odd)

    ps, ms, vs = halves(p_ref), halves(m_ref), halves(v_ref)
    for half in range(2):
        scaled = clip * g_ref[0, half]
        first_new = beta_one * ms[half] + (1.0 - beta_one) * scaled
        second_new = beta_two * vs[half] + (1.0 - beta_two) * scaled * scaled
        update = first_new * inv_first / (jnp.sqrt(second_new * inv_second) + epsilon)
        np_ref[0, half] = ps[half] - learn_rate * (update + decay_rate * ps[half])
        nm_ref[0, half] = first_new
        nv_ref[0, half] = second_new


def adam_tensor(tensor, state, grads, low, clip, partial=None):
    count = grads.shape[2]
    rows = math.gcd(count, ROWS)
    smem = pl.BlockSpec(memory_space=pltpu.SMEM)
    moved = pl.BlockSpec((2 * rows, LANES), lambda j: (j, 0))
    fresh = pl.BlockSpec((1, 2, rows, LANES), lambda j: (tensor, 0, j, 0))
    kept = list(partial) if partial is not None else []
    return pl.pallas_call(
        adam_body,
        grid=(count // rows,),
        in_specs=[smem, smem, moved, moved, moved, fresh] + [pl.BlockSpec(memory_space=pl.ANY)] * len(kept),
        out_specs=[fresh] * 3,
        out_shape=[jax.ShapeDtypeStruct(grads.shape, grads.dtype)] * 3,
        input_output_aliases={6 + i: i for i in range(len(kept))},
        compiler_params=pltpu.CompilerParams(dimension_semantics=("arbitrary",)),
        name=f"adam_{tensor}",
    )(low.reshape(1), clip.reshape(1), *state, grads, *kept)


def moved_by(key, arrays):
    if key == 0:
        return tuple(arrays)
    pairs = [(i, i ^ key) for i in range(lax.axis_size(AXES))]
    return tuple(lax.ppermute(a, AXES, pairs) for a in arrays)


def others(array, axis):
    size = lax.axis_size(axis)
    return [lax.ppermute(array, axis, [(i, i ^ key) for i in range(size)]) for key in range(1, size)]


def clip_of(total, count):
    limit = jnp.float32(0.5 * math.sqrt(count))
    return limit / jnp.maximum(jnp.sqrt(jnp.sum(total)), limit)


def shards(old_params, old_first, old_second, gradients, old_table, new_table):
    devices = lax.axis_size(AXES)
    tensors, halves, length = old_params.shape
    count = length // LANES
    old_key = old_table[:, 0]
    route = jnp.bitwise_xor(jnp.right_shift(old_key, 1), new_table[:, 0])
    low = jnp.bitwise_and(old_key, 1)
    grads = gradients.reshape(tensors, halves, count, LANES)

    def rows_of(a):
        return a.reshape(tensors, halves, count, LANES).transpose(0, 2, 1, 3).reshape(tensors, count * halves, LANES)

    state = [rows_of(a) for a in (old_params, old_first, old_second)]

    bits = devices.bit_length() - 1
    rest = [(at, min(GROUP_BITS, bits - at)) for at in range(GROUP_BITS, bits, GROUP_BITS)]
    first = min(GROUP_BITS, bits)

    def field(t, at, width):
        return jnp.bitwise_and(jnp.right_shift(route[t], at), (1 << width) - 1)

    def rest_of_way(t, mine):
        for at, width in rest:
            hops = [lambda arrays, key=key: moved_by(key << at, arrays) for key in range(1 << width)]
            mine = lax.switch(field(t, at, width), hops, mine)
        return mine

    def moved(t):
        mine = [s[t] for s in state]
        hops = [lambda arrays, key=key: moved_by(key, arrays) for key in range(1 << first)]
        return rest_of_way(t, lax.switch(field(t, 0, first), hops, mine))

    squares = jnp.sum(grads * grads, axis=(0, 1, 2)).reshape(1, LANES)
    by_row = others(squares, "row")
    ready = [moved(0)]
    ready[0], by_row = lax.optimization_barrier((ready[0], by_row))
    squares = sum(by_row, squares)
    by_col = others(squares, "col")
    ready += [moved(t) for t in range(1, tensors)]
    clip = clip_of(sum(by_col, squares), gradients.size * devices)
    outs = None
    for t in range(tensors):
        outs = adam_tensor(t, ready[t], grads, low[t], clip, outs)
    return tuple(o.reshape(gradients.shape) for o in outs)


def solution(mesh):
    spec = P(None, AXES, None)
    return jax.shard_map(
        shards,
        mesh=mesh,
        in_specs=(spec, spec, spec, spec, P(), P()),
        out_specs=(spec, spec, spec),
        check_vma=False,
    )
```
